512 devices in a mesh: space: 64 (over z, y_lo, x), mode: 8 (over y_hi, core).
Axes of the slice: x: 4, y: 8 (y_hi: 4, y_lo: 2; y = y_hi * 2 + y_lo), z: 8, core: 2. Of those that a mesh axis runs over, the one named last changes fastest.
Arguments:
- modes: float32 [3, 128, 65536], P(None, 'mode', 'space'), may hold values from -16 to 16
- stencil_coef: float32 [3, 6, 65536], P(None, None, 'space'), may hold values from -3 to 3
- volumes: float32 [65536], P('space'), may hold values from 0.5 to 2
- neighbours: int32 [6, 65536], P(None, 'space'), may hold values from 0 to 65535, as said below
Outputs:
- tensor: float32 [128, 128, 128], P('mode', 'space')
The draws below stay inside these ranges and needn't reach their ends.
Inputs may be any that keep to these rules, and one draw needn't show every extreme that they name: `neighbours`: each entry differs from its own cell's index by 1 to 128.
All inputs are finite; a program needn't handle non-finite values.
Results may differ from the reference program's by a relative error of at most 0.005.
Values may be sent and summed in bfloat16 or wider, within the bound.
No kernel may reach another device: no remote copies, remote signals or barrier semaphores. Data moves between devices by JAX's collectives and lax.ppermute only.
A program may use at most 64 MiB of HBM per device.

```python
import math
import jax
import jax.numpy as jnp
from jax import lax

MODES = 128
NB = 6
HALO = 128
CELLS = 65536


def draw_neighbours(key, part):
    first, second = jax.random.split(jax.random.fold_in(key, 11))
    distance = jax.random.randint(first, (NB, CELLS), 1, HALO + 1)
    sign = jax.random.randint(second, (NB, CELLS), 0, 2) * 2 - 1
    place = jnp.arange(CELLS, dtype=jnp.int32)[None, :]
    target = place + sign * distance
    outside = (target < 0) | (target >= CELLS)
    target = jnp.where(outside, place - sign * distance, target)
    return target.astype(jnp.int32)


def spiked(array, key, source, target, shards_of, factor):
    owner, partner = [(jnp.arange(array.shape[axis_at]) // (array.shape[axis_at] // shards_of)).reshape([-1 if axis == axis_at else 1 for axis in range(array.ndim)]) for axis_at in (source, target)]
    chosen = jax.random.permutation(key, shards_of)[partner]
    strong = (owner == chosen) | (owner == (partner + shards_of // 2) % shards_of)
    return jnp.where(strong, factor * array, array)


def level_of(rng, dims, cuts, low, top_value):
    def one(position, shards_of):
        heights = jax.random.uniform(jax.random.fold_in(jax.random.fold_in(rng, 6), position), (shards_of,), jnp.float32, low / len(cuts), top_value / len(cuts))
        return jnp.repeat(jnp.exp(heights), dims[position] // shards_of).reshape((-1,) + (1,) * (len(dims) - position - 1))

    level = one(*cuts[0])
    for cut in cuts[1:]:
        level = level * one(*cut)
    return level


def gaussian(rng, shape, deviation, bound, cuts=(), kind=jnp.bfloat16):
    factor_of = level_of(rng, shape, cuts, -0.22, 0.18) if cuts else 1.0
    entries = jax.random.normal(rng, shape, jnp.float32) * deviation * factor_of
    return jnp.minimum(jnp.maximum(entries, -bound), bound).astype(kind)


def bell_draw_with(key, extent, scale, reach, cuts, heavy, held_as=jnp.bfloat16):
    values = scale * jax.random.normal(key, extent, jnp.float32)
    if cuts:
        values = values * level_of(key, extent, cuts, -0.22, 0.18)
    return jnp.clip(spiked(values, jax.random.fold_in(key, 3), *heavy), -reach, reach).astype(held_as)


def setup_inputs(seed: int = 0) -> dict:
    key_list = jax.random.split(jax.random.key(seed), 5)
    modes = bell_draw_with(key_list[0], (3, MODES, CELLS), 1.0, 16.0, ((1, 8), (2, 64)), (2, 1, 64, 4.0), jnp.float32)
    stencil_coef = gaussian(key_list[1], (3, NB, CELLS), 0.5, 3.0, ((2, 64),), jnp.float32)
    volumes = jnp.clip(jnp.exp(math.log(2.0) - 1.3862944 * jax.random.uniform(key_list[2], (CELLS,), jnp.float32) ** level_of(key_list[2], (CELLS,), ((0, 64),), -0.2, 0.2)), 0.5, 2.0)
    neighbours = draw_neighbours(jax.random.fold_in(key_list[4], 71), 0)
    return dict(modes=modes, stencil_coef=stencil_coef, volumes=volumes, neighbours=neighbours)


def reference(modes, stencil_coef, volumes, neighbours):
    low = modes.astype(jnp.bfloat16)
    flat_low = jnp.transpose(low, (1, 0, 2)).reshape(MODES, 3 * CELLS)
    weight = volumes * (1.0 / math.sqrt(CELLS))

    def per_mode(index):
        field = lax.dynamic_index_in_dim(modes, index, 1, keepdims=False)
        near = field[:, neighbours]
        grads = stencil_coef[:, 0][:, None, :] * (near[:, 0] - field)[None]
        for step in range(1, NB):
            grads = grads + stencil_coef[:, step][:, None, :] * (near[:, step] - field)[None]
        mixed = low[0].astype(jnp.float32)[:, None, :] * grads[0][None]
        mixed = mixed + low[1].astype(jnp.float32)[:, None, :] * grads[1][None]
        mixed = mixed + low[2].astype(jnp.float32)[:, None, :] * grads[2][None]
        carried = (mixed * weight[None, None, :]).astype(jnp.bfloat16).reshape(MODES, 3 * CELLS)
        return lax.dot_general(flat_low, carried, (((1,), (1,)), ((), ())), preferred_element_type=jnp.float32)
    return lax.map(per_mode, jnp.arange(MODES, dtype=jnp.int32))
```

```python
import math

import jax
import jax.numpy as jnp
from jax import lax
from jax.experimental import pallas as pl
from jax.experimental.pallas import tpu as pltpu
from jax.sharding import Mesh, PartitionSpec as P

SPACE = ("z", "ylo", "x")
MODE = ("yhi", "core")
PLANE = ("ylo", "x")
GROUP = 4
LANES = 128
TILE = 32


def picked(block, lane):
    return jnp.take_along_axis(block, lane, axis=1, mode="promise_in_bounds")


def grads_kernel(scale, near_ref, coef_ref, vol_ref, left_ref, mid_ref, right_ref, out_ref):
    comps, count, width = mid_ref.shape
    dirs, steps = coef_ref.shape[:2]
    tiles = width // LANES
    for t in range(tiles):
        at = slice(t * LANES, (t + 1) * LANES)
        weight = vol_ref[:, at] * scale
        lanes, ahead, behind, coefs = [], [], [], []
        for n in range(steps):
            index = jnp.broadcast_to(near_ref[n : n + 1, at], (8, LANES))
            lanes.append(index & (LANES - 1))
            apart = ((index >> 7) - t) & 3
            ahead.append(apart == 1)
            behind.append(apart == 3)
            coefs.append(
                [jnp.broadcast_to(coef_ref[d, n : n + 1, at] * weight, (8, LANES)) for d in range(dirs)]
            )
        for c in range(comps):
            for r in range(0, count, 8):
                rows = slice(r, r + 8)
                here = mid_ref[c, rows, at]
                if t == 0:
                    before = left_ref[c, rows, :]
                else:
                    before = mid_ref[c, rows, (t - 1) * LANES : t * LANES]
                if t == tiles - 1:
                    after = right_ref[c, rows, :]
                else:
                    after = mid_ref[c, rows, (t + 1) * LANES : (t + 2) * LANES]
                total = [None] * dirs
                for n in range(steps):
                    near = jnp.where(
                        ahead[n],
                        picked(after, lanes[n]),
                        jnp.where(behind[n], picked(before, lanes[n]), picked(here, lanes[n])),
                    )
                    change = near - here
                    for d in range(dirs):
                        term = coefs[n][d] * change
                        total[d] = term if total[d] is None else total[d] + term
                for d in range(dirs):
                    out_ref[pl.ds((d * comps + c) * count + r, 8), at] = total[d]


def weighted_grads(modes, left, right, stencil_coef, volumes, neighbours, scale):
    comps, count, width = modes.shape
    return pl.pallas_call(
        lambda *refs: grads_kernel(scale, *refs),
        out_shape=jax.ShapeDtypeStruct((9 * count, width), jnp.float32),
        in_specs=[pl.BlockSpec(memory_space=pltpu.VMEM)] * 6,
        out_specs=pl.BlockSpec(memory_space=pltpu.VMEM),
        compiler_params=pltpu.CompilerParams(vmem_limit_bytes=4 << 20),
        cost_estimate=pl.CostEstimate(flops=8_000_000, bytes_accessed=1_000_000, transcendentals=0),
        name="grads",
    )(neighbours, stencil_coef, volumes.reshape(1, width), left, modes, right)


def tensor_kernel(grad_ref, own_ref, other_ref, out_ref, wide_ref, flat_ref, held_a, held_b, rows_ref):
    chips, comps, count, width = own_ref.shape
    blocks = 2 * chips
    total = blocks * count
    core = lax.axis_index("core")
    for c in range(comps):
        for h, ref in ((0, own_ref), (1, other_ref)):
            place = core if h == 0 else 1 - core
            for y in range(chips):
                row = pl.multiple_of((2 * y + place) * count, count)
                piece = ref[y, c]
                flat_ref[pl.ds(row, count), pl.ds(c * width, width)] = piece
                wide_ref[c, pl.ds(row, count), :] = piece.astype(jnp.float32)

    def build(group, held):
        for x in range(0, width, LANES):
            at = slice(x, x + LANES)
            for j in range(0, total, TILE):
                low = [wide_ref[d, j : j + TILE, at] for d in range(3)]
                for kk in range(GROUP):
                    k = group * GROUP + kk
                    for c in range(comps):
                        row = [grad_ref[pl.ds((d * comps + c) * count + k, 1), at] for d in range(3)]
                        mixed = low[0] * row[0] + low[1] * row[1] + low[2] * row[2]
                        held[kk * total + j : kk * total + j + TILE, c * width + x : c * width + x + LANES] = (
                            mixed.astype(jnp.bfloat16)
                        )

    def contract(group, held):
        part = lax.dot_general(
            held[...], flat_ref[...], (((1,), (1,)), ((), ())), preferred_element_type=jnp.float32
        )
        for kk in range(GROUP):
            k = group * GROUP + kk
            rows_ref[pl.ds(k, total, stride=count), :] = part[kk * total : (kk + 1) * total].T

    groups = count // GROUP
    helds = (held_a, held_b)
    build(0, helds[0])
    for g in range(groups):
        if g + 1 < groups:
            build(g + 1, helds[(g + 1) % 2])
        contract(g, helds[g % 2])
    first, second, size = out_ref.shape[:3]
    for a in range(first):
        for b in range(second):
            out_ref[a, b] = rows_ref[pl.ds((b * first + a) * size, size), :].astype(jnp.bfloat16)


def local_tensor(grads, own, other, plane, depth):
    chips, comps, count, width = own.shape
    total = 2 * chips * count
    rows = 2 * count
    return pl.pallas_call(
        tensor_kernel,
        out_shape=jax.ShapeDtypeStruct((plane, depth, rows, total), jnp.bfloat16),
        in_specs=[pl.BlockSpec(memory_space=pltpu.VMEM)] * 3,
        out_specs=pl.BlockSpec(memory_space=pltpu.VMEM),
        scratch_shapes=[
            pltpu.VMEM((comps, total, width), jnp.float32),
            pltpu.VMEM((total, comps * width), jnp.bfloat16),
            pltpu.VMEM((GROUP * total, comps * width), jnp.bfloat16),
            pltpu.VMEM((GROUP * total, comps * width), jnp.bfloat16),
            pltpu.VMEM((count * total, total), jnp.float32),
        ],
        compiler_params=pltpu.CompilerParams(vmem_limit_bytes=16 << 20),
        cost_estimate=pl.CostEstimate(flops=1_700_000_000, bytes_accessed=2_000_000, transcendentals=0),
        name="tensor",
    )(grads, own, other)


def sum_kernel(tiles_ref, out_ref):
    total = tiles_ref[0].astype(jnp.float32)
    for i in range(1, tiles_ref.shape[0]):
        total = total + tiles_ref[i].astype(jnp.float32)
    out_ref[...] = total.astype(out_ref.dtype)


def summed(tiles, dtype):
    return pl.pallas_call(
        sum_kernel,
        out_shape=jax.ShapeDtypeStruct(tiles.shape[1:], dtype),
        in_specs=[pl.BlockSpec(memory_space=pltpu.VMEM)],
        out_specs=pl.BlockSpec(memory_space=pltpu.VMEM),
        compiler_params=pltpu.CompilerParams(vmem_limit_bytes=4 << 20),
        cost_estimate=pl.CostEstimate(flops=300_000, bytes_accessed=600_000, transcendentals=0),
        name="summed",
    )(tiles)


def body(modes, stencil_coef, volumes, neighbours):
    comps, count, width = modes.shape
    cells = width * lax.axis_size(SPACE)
    low = modes.astype(jnp.bfloat16)
    chips = lax.axis_size("yhi")
    copies = jnp.broadcast_to(low, (chips, *low.shape))
    own = lax.all_to_all(copies, "yhi", 0, 0, tiled=True)
    last = lax.axis_size(SPACE) - 1
    left = lax.ppermute(modes[:, :, width - LANES :], SPACE, [(i, i + 1) for i in range(last)])
    right = lax.ppermute(modes[:, :, :LANES], SPACE, [(i + 1, i) for i in range(last)])
    grads = weighted_grads(modes, left, right, stencil_coef, volumes, neighbours, 1.0 / math.sqrt(cells))
    other = lax.ppermute(own, "core", [(0, 1), (1, 0)])
    plane, depth = lax.axis_size(PLANE), lax.axis_size("z")
    share = local_tensor(grads, own, other, plane, depth)
    first = lax.all_to_all(share, PLANE, 0, 0, tiled=True)
    partial = summed(first, jnp.bfloat16)
    second = lax.all_to_all(partial, "z", 0, 0, tiled=True)
    rows = summed(second, jnp.float32)
    return jnp.transpose(rows.reshape(2, count, -1), (1, 0, 2))


def solution(mesh):
    sizes = (8, 2, 4, 4, 2)
    fine = Mesh(mesh.devices.reshape(sizes), SPACE + MODE)
    in_specs = (P(None, MODE, SPACE), P(None, None, SPACE), P(SPACE), P(None, SPACE))
    out_specs = P(MODE, SPACE, None)
    return jax.shard_map(body, mesh=fine, in_specs=in_specs, out_specs=out_specs, check_vma=False)
```

```python
import math

import jax
import jax.numpy as jnp
from jax import lax
from jax.experimental import pallas as pl
from jax.experimental.pallas import tpu as pltpu
from jax.sharding import Mesh, PartitionSpec as P

SPACE = ("z", "ylo", "x")
MODE = ("yhi", "core")
PLANE = ("ylo", "x")
GROUP = 4
WIDE = 256
LANES = 128
TILE = 16


def picked(block, lane):
    return jnp.take_along_axis(block, lane, axis=1, mode="promise_in_bounds")


def grads_kernel(scale, near_ref, coef_ref, vol_ref, left_ref, mid_ref, right_ref, out_ref):
    comps, count, width = mid_ref.shape
    dirs, steps = coef_ref.shape[:2]
    tiles = width // LANES
    for t in range(tiles):
        at = slice(t * LANES, (t + 1) * LANES)
        weight = vol_ref[:, at] * scale
        lanes, ahead, behind, coefs = [], [], [], []
        for n in range(steps):
            index = jnp.broadcast_to(near_ref[n : n + 1, at], (8, LANES))
            lanes.append(index & (LANES - 1))
            apart = ((index >> 7) - t) & 3
            ahead.append(apart == 1)
            behind.append(apart == 3)
            coefs.append(
                [jnp.broadcast_to(coef_ref[d, n : n + 1, at] * weight, (8, LANES)) for d in range(dirs)]
            )
        for c in range(comps):
            for r in range(0, count, 8):
                rows = slice(r, r + 8)
                here = mid_ref[c, rows, at]
                if t == 0:
                    before = left_ref[c, rows, :]
                else:
                    before = mid_ref[c, rows, (t - 1) * LANES : t * LANES]
                if t == tiles - 1:
                    after = right_ref[c, rows, :]
                else:
                    after = mid_ref[c, rows, (t + 1) * LANES : (t + 2) * LANES]
                total = [None] * dirs
                for n in range(steps):
                    near = jnp.where(
                        ahead[n],
                        picked(after, lanes[n]),
                        jnp.where(behind[n], picked(before, lanes[n]), picked(here, lanes[n])),
                    )
                    change = near - here
                    for d in range(dirs):
                        term = coefs[n][d] * change
                        total[d] = term if total[d] is None else total[d] + term
                for d in range(dirs):
                    out_ref[pl.ds((d * comps + c) * count + r, 8), at] = total[d]


def weighted_grads(modes, left, right, stencil_coef, volumes, neighbours, scale):
    comps, count, width = modes.shape
    return pl.pallas_call(
        lambda *refs: grads_kernel(scale, *refs),
        out_shape=jax.ShapeDtypeStruct((9 * count, width), jnp.float32),
        in_specs=[pl.BlockSpec(memory_space=pltpu.VMEM)] * 6,
        out_specs=pl.BlockSpec(memory_space=pltpu.VMEM),
        compiler_params=pltpu.CompilerParams(vmem_limit_bytes=4 << 20),
        cost_estimate=pl.CostEstimate(flops=8_000_000, bytes_accessed=1_000_000, transcendentals=0),
        name="grads",
    )(neighbours, stencil_coef, volumes.reshape(1, width), left, modes, right)


def tensor_kernel(flat_order, *refs):
    grad_ref, lows = refs[0], refs[1:-6]
    out_ref, wide_ref, flat_ref, held_a, held_b, rows_ref = refs[-6:]
    chips, comps, count, width = lows[0].shape
    total = sum(ref.shape[0] for ref in lows) * count
    core = 0 if flat_order else lax.axis_index("core")
    for c in range(comps):
        for h, ref in enumerate(lows):
            for y in range(chips):
                if flat_order:
                    row = y * count
                else:
                    row = pl.multiple_of((2 * y + (core if h == 0 else 1 - core)) * count, count)
                piece = ref[y, c]
                flat_ref[pl.ds(row, count), pl.ds(c * width, width)] = piece
                wide_ref[c, pl.ds(row, count), :] = piece.astype(jnp.float32)

    def build(group, x, c, held):
        at = slice(x, x + WIDE)
        for j in range(0, total, TILE):
            low = [wide_ref[d, j : j + TILE, at] for d in range(3)]
            for kk in range(GROUP):
                k = group * GROUP + kk
                row = [grad_ref[pl.ds((d * comps + c) * count + k, 1), at] for d in range(3)]
                mixed = low[0] * row[0] + low[1] * row[1] + low[2] * row[2]
                held[kk * total + j : kk * total + j + TILE, :] = mixed.astype(jnp.bfloat16)

    def contract(x, c, held, part):
        more = lax.dot_general(
            held[...],
            flat_ref[:, c * width + x : c * width + x + WIDE],
            (((1,), (1,)), ((), ())),
            preferred_element_type=jnp.float32,
        )
        return more if part is None else part + more

    def finish(group, part):
        for kk in range(GROUP):
            k = group * GROUP + kk
            rows_ref[pl.ds(k, total, stride=count), :] = part[kk * total : (kk + 1) * total].T

    helds = (held_a, held_b)
    work = [(g, x, c) for g in range(count // GROUP) for x in range(0, width, WIDE) for c in range(comps)]
    each = len(work) // (count // GROUP)
    build(*work[0], helds[0])
    part = None
    for n, (g, x, c) in enumerate(work):
        if n + 1 < len(work):
            build(*work[n + 1], helds[(n + 1) % 2])
        part = contract(x, c, helds[n % 2], part)
        if n % each == each - 1:
            finish(g, part)
            part = None
    first, second, size = out_ref.shape[:3]
    for a in range(first):
        for b in range(second):
            out_ref[a, b] = rows_ref[pl.ds((a * second + b) * size, size), :].astype(jnp.bfloat16)


def local_tensor(grads, lows, plane, depth):
    comps, count, width = lows[0].shape[1:]
    total = sum(low.shape[0] for low in lows) * count
    rows = 2 * count
    return pl.pallas_call(
        lambda *refs: tensor_kernel(len(lows) == 1, *refs),
        out_shape=jax.ShapeDtypeStruct((plane, depth, rows, total), jnp.bfloat16),
        in_specs=[pl.BlockSpec(memory_space=pltpu.VMEM)] * (1 + len(lows)),
        out_specs=pl.BlockSpec(memory_space=pltpu.VMEM),
        scratch_shapes=[
            pltpu.VMEM((comps, total, width), jnp.float32),
            pltpu.VMEM((total, comps * width), jnp.bfloat16),
            pltpu.VMEM((GROUP * total, WIDE), jnp.bfloat16),
            pltpu.VMEM((GROUP * total, WIDE), jnp.bfloat16),
            pltpu.VMEM((count * total, total), jnp.float32),
        ],
        compiler_params=pltpu.CompilerParams(vmem_limit_bytes=16 << 20),
        cost_estimate=pl.CostEstimate(flops=1_700_000_000, bytes_accessed=2_000_000, transcendentals=0),
        name="tensor",
    )(grads, *lows)


def placed_kernel(tiles_ref, out_ref):
    total = tiles_ref[0].astype(jnp.float32)
    for i in range(1, tiles_ref.shape[0]):
        total = total + tiles_ref[i].astype(jnp.float32)
    count, pairs = out_ref.shape[:2]
    for i in range(pairs):
        out_ref[:, i, :] = total[i * count : (i + 1) * count]


def placed(tiles, count):
    rows, total = tiles.shape[1:]
    return pl.pallas_call(
        placed_kernel,
        out_shape=jax.ShapeDtypeStruct((count, rows // count, total), jnp.float32),
        in_specs=[pl.BlockSpec(memory_space=pltpu.VMEM)],
        out_specs=pl.BlockSpec(memory_space=pltpu.VMEM),
        compiler_params=pltpu.CompilerParams(vmem_limit_bytes=4 << 20),
        name="placed",
    )(tiles)


def body(modes, stencil_coef, volumes, neighbours):
    comps, count, width = modes.shape
    cells = width * lax.axis_size(SPACE)
    low = modes.astype(jnp.bfloat16)
    chips = lax.axis_size("yhi")
    copies = jnp.broadcast_to(low, (chips, *low.shape))
    own = lax.all_to_all(copies, "yhi", 0, 0, tiled=True)
    last = lax.axis_size(SPACE) - 1
    left = lax.ppermute(modes[:, :, width - LANES :], SPACE, [(i, i + 1) for i in range(last)])
    right = lax.ppermute(modes[:, :, :LANES], SPACE, [(i + 1, i) for i in range(last)])
    grads = weighted_grads(modes, left, right, stencil_coef, volumes, neighbours, 1.0 / math.sqrt(cells))
    own, grads = lax.optimization_barrier((own, grads))
    other = lax.ppermute(own, "core", [(0, 1), (1, 0)])
    lows = (own, other)
    plane, depth = lax.axis_size(PLANE), lax.axis_size("z")
    share = local_tensor(grads, lows, plane, depth)
    second = lax.all_to_all(share.reshape(plane * depth, 2 * count, -1), SPACE, 0, 0, tiled=True)
    return placed(second, count)


def solution(mesh):
    sizes = (8, 2, 4, 4, 2)
    fine = Mesh(mesh.devices.reshape(sizes), SPACE + MODE)
    in_specs = (P(None, MODE, SPACE), P(None, None, SPACE), P(SPACE), P(None, SPACE))
    out_specs = P(MODE, SPACE, None)
    return jax.shard_map(body, mesh=fine, in_specs=in_specs, out_specs=out_specs, check_vma=False)
```

```python
import math

import jax
import jax.numpy as jnp
from jax import lax
from jax.experimental import pallas as pl
from jax.experimental.pallas import tpu as pltpu
from jax.sharding import Mesh, PartitionSpec as P

SPACE = ("z", "ylo", "x")
MODE = ("yhi", "core")
GROUP = 4
WIDE = 256
LANES = 128
TILE = 16


def picked(block, lane):
    return jnp.take_along_axis(block, lane, axis=1, mode="promise_in_bounds")


def grads_kernel(scale, near_ref, coef_ref, vol_ref, left_ref, mid_ref, right_ref, out_ref):
    comps, count, width = mid_ref.shape
    dirs, steps = coef_ref.shape[:2]
    tiles = width // LANES
    for t in range(tiles):
        at = slice(t * LANES, (t + 1) * LANES)
        weight = vol_ref[:, at] * scale
        lanes, ahead, behind, coefs = [], [], [], []
        for n in range(steps):
            index = jnp.broadcast_to(near_ref[n : n + 1, at], (8, LANES))
            lanes.append(index & (LANES - 1))
            apart = ((index >> 7) - t) & 3
            ahead.append(apart == 1)
            behind.append(apart == 3)
            coefs.append(
                [jnp.broadcast_to(coef_ref[d, n : n + 1, at] * weight, (8, LANES)) for d in range(dirs)]
            )
        for c in range(comps):
            for r in range(0, count, 8):
                rows = slice(r, r + 8)
                here = mid_ref[c, rows, at]
                if t == 0:
                    before = left_ref[c, rows, :]
                else:
                    before = mid_ref[c, rows, (t - 1) * LANES : t * LANES]
                if t == tiles - 1:
                    after = right_ref[c, rows, :]
                else:
                    after = mid_ref[c, rows, (t + 1) * LANES : (t + 2) * LANES]
                total = [None] * dirs
                for n in range(steps):
                    near = jnp.where(
                        ahead[n],
                        picked(after, lanes[n]),
                        jnp.where(behind[n], picked(before, lanes[n]), picked(here, lanes[n])),
                    )
                    change = near - here
                    for d in range(dirs):
                        term = coefs[n][d] * change
                        total[d] = term if total[d] is None else total[d] + term
                for d in range(dirs):
                    out_ref[pl.ds((d * comps + c) * count + r, 8), at] = total[d]


def weighted_grads(modes, left, right, stencil_coef, volumes, neighbours, scale):
    comps, count, width = modes.shape
    return pl.pallas_call(
        lambda *refs: grads_kernel(scale, *refs),
        out_shape=jax.ShapeDtypeStruct((9 * count, width), jnp.float32),
        in_specs=[pl.BlockSpec(memory_space=pltpu.VMEM)] * 6,
        out_specs=pl.BlockSpec(memory_space=pltpu.VMEM),
        compiler_params=pltpu.CompilerParams(vmem_limit_bytes=4 << 20),
        cost_estimate=pl.CostEstimate(flops=8_000_000, bytes_accessed=1_000_000, transcendentals=0),
        name="grads",
    )(neighbours, stencil_coef, volumes.reshape(1, width), left, modes, right)


def tensor_kernel(absolute, grad_ref, own_ref, other_ref, out_ref, wide_ref, flat_ref, held_a, held_b, rows_ref):
    chips, comps, count, width = own_ref.shape
    blocks = 2 * chips
    total = blocks * count

    def spread(x):
        for y in range(chips):
            for h, ref in enumerate((own_ref, other_ref)):
                rows = slice((2 * y + h) * count, (2 * y + h + 1) * count)
                for c in range(comps):
                    piece = ref[y, c, :, x : x + WIDE]
                    flat_ref[rows, c * width + x : c * width + x + WIDE] = piece
                    wide_ref[c, rows, x : x + WIDE] = piece.astype(jnp.float32)

    def build(group, x, c, held):
        if group == 0 and c == 0:
            spread(x)
        at = slice(x, x + WIDE)
        for j in range(0, total, TILE):
            low = [wide_ref[d, j : j + TILE, at] for d in range(3)]
            for kk in range(GROUP):
                k = group * GROUP + kk
                row = [grad_ref[pl.ds((d * comps + c) * count + k, 1), at] for d in range(3)]
                mixed = low[0] * row[0] + low[1] * row[1] + low[2] * row[2]
                held[kk * total + j : kk * total + j + TILE, :] = mixed.astype(jnp.bfloat16)

    def contract(x, c, held, part):
        more = lax.dot_general(
            held[...],
            flat_ref[:, c * width + x : c * width + x + WIDE],
            (((1,), (1,)), ((), ())),
            preferred_element_type=jnp.float32,
        )
        return more if part is None else part + more

    def finish(group, part):
        for kk in range(GROUP):
            k = group * GROUP + kk
            rows_ref[pl.ds(k, total, stride=count), :] = part[kk * total : (kk + 1) * total].T

    helds = (held_a, held_b)
    work = [(g, x, c) for g in range(count // GROUP) for x in range(0, width, WIDE) for c in range(comps)]
    each = len(work) // (count // GROUP)
    build(*work[0], helds[0])
    part = None
    for n, (g, x, c) in enumerate(work):
        if n + 1 < len(work):
            build(*work[n + 1], helds[(n + 1) % 2])
        part = contract(x, c, helds[n % 2], part)
        if n % each == each - 1:
            finish(g, part)
            part = None
    size = out_ref.shape[1]
    each = out_ref.shape[0] // blocks
    for r in range(blocks):
        rows = rows_ref[r * each * size : (r + 1) * each * size, :].astype(jnp.bfloat16)
        out_ref[pl.ds(absolute(r) * each, each)] = rows.reshape(each, size, total)


def local_tensor(grads, own, other, shards, absolute):
    chips, comps, count, width = own.shape
    total = 2 * chips * count
    return pl.pallas_call(
        lambda *refs: tensor_kernel(absolute, *refs),
        out_shape=jax.ShapeDtypeStruct((shards, total * count // shards, total), jnp.bfloat16),
        in_specs=[pl.BlockSpec(memory_space=pltpu.VMEM)] * 3,
        out_specs=pl.BlockSpec(memory_space=pltpu.VMEM),
        scratch_shapes=[
            pltpu.VMEM((comps, total, width), jnp.float32),
            pltpu.VMEM((total, comps * width), jnp.bfloat16),
            pltpu.VMEM((GROUP * total, WIDE), jnp.bfloat16),
            pltpu.VMEM((GROUP * total, WIDE), jnp.bfloat16),
            pltpu.VMEM((count * total, total), jnp.float32),
        ],
        compiler_params=pltpu.CompilerParams(vmem_limit_bytes=16 << 20),
        cost_estimate=pl.CostEstimate(flops=1_700_000_000, bytes_accessed=2_000_000, transcendentals=0),
        name="tensor",
    )(grads, own, other)


def placed_kernel(relative, tiles_ref, out_ref):
    total = tiles_ref[0].astype(jnp.float32)
    for i in range(1, tiles_ref.shape[0]):
        total = total + tiles_ref[i].astype(jnp.float32)
    count, pairs, modes = out_ref.shape
    place = lax.broadcasted_iota(jnp.int32, (8, modes), 1)
    lane = relative(place >> 4) * 16 + (place & 15)
    for i in range(pairs):
        for r in range(0, count, 8):
            out_ref[r : r + 8, i, :] = picked(total[i * count + r : i * count + r + 8], lane)


def placed(tiles, count, relative):
    rows, total = tiles.shape[1:]
    return pl.pallas_call(
        lambda *refs: placed_kernel(relative, *refs),
        out_shape=jax.ShapeDtypeStruct((count, rows // count, total), jnp.float32),
        in_specs=[pl.BlockSpec(memory_space=pltpu.VMEM)],
        out_specs=pl.BlockSpec(memory_space=pltpu.VMEM),
        compiler_params=pltpu.CompilerParams(vmem_limit_bytes=4 << 20),
        name="placed",
    )(tiles)


def body(modes, stencil_coef, volumes, neighbours):
    comps, count, width = modes.shape
    cells = width * lax.axis_size(SPACE)
    low = modes.astype(jnp.bfloat16)
    chips = lax.axis_size("yhi")
    copies = jnp.broadcast_to(low, (chips, *low.shape))
    own = lax.all_to_all(copies, "yhi", 0, 0, tiled=True)
    last = lax.axis_size(SPACE) - 1
    left = lax.ppermute(modes[:, :, width - LANES :], SPACE, [(i, i + 1) for i in range(last)])
    right = lax.ppermute(modes[:, :, :LANES], SPACE, [(i + 1, i) for i in range(last)])
    grads = weighted_grads(modes, left, right, stencil_coef, volumes, neighbours, 1.0 / math.sqrt(cells))
    own, grads = lax.optimization_barrier((own, grads))
    other = lax.ppermute(own, "core", [(0, 1), (1, 0)])
    def swapped(block):
        return block ^ lax.axis_index("core")

    absolute, relative = swapped, swapped
    share = local_tensor(grads, own, other, lax.axis_size(SPACE), absolute)
    tiles = lax.all_to_all(share, SPACE, 0, 0, tiled=True)
    return placed(tiles, count, relative)


def solution(mesh):
    sizes = (8, 2, 4, 4, 2)
    fine = Mesh(mesh.devices.reshape(sizes), SPACE + MODE)
    in_specs = (P(None, MODE, SPACE), P(None, None, SPACE), P(SPACE), P(None, SPACE))
    out_specs = P(MODE, SPACE, None)
    return jax.shard_map(body, mesh=fine, in_specs=in_specs, out_specs=out_specs, check_vma=False)
```

```python
import math

import jax
import jax.numpy as jnp
from jax import lax
from jax.experimental import pallas as pl
from jax.experimental.pallas import tpu as pltpu
from jax.sharding import Mesh, PartitionSpec as P

SPACE = ("z", "ylo", "x")
MODE = ("yhi", "core")
GROUP = 4
WIDE = 256
LANES = 128
TILE = 16
EARLY = 3


def picked(block, lane):
    return jnp.take_along_axis(block, lane, axis=1, mode="promise_in_bounds")


def grads_kernel(scale, near_ref, coef_ref, vol_ref, even_ref, mid_ref, odd_ref, out_ref):
    comps, count, width = mid_ref.shape
    dirs, steps = coef_ref.shape[:2]
    tiles = width // LANES
    odd = (lax.axis_index("x") & 1) == 1
    for t in range(tiles):
        at = slice(t * LANES, (t + 1) * LANES)
        weight = vol_ref[:, at] * scale
        lanes, ahead, behind, coefs = [], [], [], []
        for n in range(steps):
            index = jnp.broadcast_to(near_ref[n : n + 1, at], (8, LANES))
            lanes.append(index & (LANES - 1))
            apart = ((index >> 7) - t) & 3
            ahead.append(apart == 1)
            behind.append(apart == 3)
            coefs.append(
                [jnp.broadcast_to(coef_ref[d, n : n + 1, at] * weight, (8, LANES)) for d in range(dirs)]
            )
        for c in range(comps):
            for r in range(0, count, 8):
                rows = slice(r, r + 8)
                here = mid_ref[c, rows, at]
                if t == 0:
                    before = jnp.where(odd, even_ref[c, rows, :], odd_ref[c, rows, :])
                else:
                    before = mid_ref[c, rows, (t - 1) * LANES : t * LANES]
                if t == tiles - 1:
                    after = jnp.where(odd, odd_ref[c, rows, :], even_ref[c, rows, :])
                else:
                    after = mid_ref[c, rows, (t + 1) * LANES : (t + 2) * LANES]
                total = [None] * dirs
                for n in range(steps):
                    near = jnp.where(
                        ahead[n],
                        picked(after, lanes[n]),
                        jnp.where(behind[n], picked(before, lanes[n]), picked(here, lanes[n])),
                    )
                    change = near - here
                    for d in range(dirs):
                        term = coefs[n][d] * change
                        total[d] = term if total[d] is None else total[d] + term
                for d in range(dirs):
                    out_ref[pl.ds((d * comps + c) * count + r, 8), at] = total[d]


def weighted_grads(modes, left, right, stencil_coef, volumes, neighbours, scale):
    _, count, width = modes.shape
    return pl.pallas_call(
        lambda *refs: grads_kernel(scale, *refs),
        out_shape=jax.ShapeDtypeStruct((9 * count, width), jnp.float32),
        in_specs=[pl.BlockSpec(memory_space=pltpu.VMEM)] * 6,
        out_specs=pl.BlockSpec(memory_space=pltpu.VMEM),
        compiler_params=pltpu.CompilerParams(vmem_limit_bytes=4 << 20),
        cost_estimate=pl.CostEstimate(flops=8_000_000, bytes_accessed=1_000_000, transcendentals=0),
        name="grads",
    )(neighbours, stencil_coef, volumes.reshape(1, width), left, modes, right)


def early_kernel(grad_ref, own_ref, *out_refs):
    chips, comps, count, width = own_ref.shape
    for x in range(0, width, WIDE):
        at = slice(x, x + WIDE)
        for y in range(chips):
            low = [own_ref[y, d, :, at].astype(jnp.float32) for d in range(3)]
            for k in range(0, count):
                group, kk = divmod(k, GROUP)
                if kk >= EARLY:
                    continue
                for c in range(comps):
                    row = [grad_ref[pl.ds((d * comps + c) * count + k, 1), at] for d in range(3)]
                    mixed = low[0] * row[0] + low[1] * row[1] + low[2] * row[2]
                    out_refs[kk][group, c, y * count : (y + 1) * count, at] = mixed.astype(jnp.bfloat16)


def early_part(grads, own):
    chips, comps, count, width = own.shape
    return pl.pallas_call(
        early_kernel,
        out_shape=[jax.ShapeDtypeStruct((count // GROUP, comps, chips * count, width), jnp.bfloat16)] * EARLY,
        in_specs=[pl.BlockSpec(memory_space=pltpu.VMEM)] * 2,
        out_specs=[pl.BlockSpec(memory_space=pltpu.VMEM)] * EARLY,
        compiler_params=pltpu.CompilerParams(vmem_limit_bytes=8 << 20),
        cost_estimate=pl.CostEstimate(flops=20_000_000, bytes_accessed=2_000_000, transcendentals=0),
        name="early",
    )(grads, own)


def tensor_kernel(absolute, grad_ref, own_ref, other_ref, *refs):
    early_refs = refs[:EARLY]
    out_ref, wide_ref, flat_ref, held_a, held_b, rows_ref = refs[EARLY:]
    chips, comps, count, width = own_ref.shape
    blocks = 2 * chips
    total = blocks * count

    def spread(x):
        for y in range(chips):
            for h, ref in enumerate((own_ref, other_ref)):
                rows = slice((2 * y + h) * count, (2 * y + h + 1) * count)
                for c in range(comps):
                    piece = ref[y, c, :, x : x + WIDE]
                    flat_ref[rows, c * width + x : c * width + x + WIDE] = piece
                    wide_ref[c, rows, x : x + WIDE] = piece.astype(jnp.float32)

    def build(group, x, c, held):
        if group == 0 and c == 0:
            spread(x)
        at = slice(x, x + WIDE)
        for j in range(0, total, TILE):
            low = [wide_ref[d, j : j + TILE, at] for d in range(3)]
            for kk in range(GROUP):
                block = j // count
                if kk < EARLY and block % 2 == 0:
                    place = block // 2 * count
                    held[kk * total + j : kk * total + j + TILE, :] = early_refs[kk][group, c, place : place + TILE, at]
                    continue
                k = group * GROUP + kk
                row = [grad_ref[pl.ds((d * comps + c) * count + k, 1), at] for d in range(3)]
                mixed = low[0] * row[0] + low[1] * row[1] + low[2] * row[2]
                held[kk * total + j : kk * total + j + TILE, :] = mixed.astype(jnp.bfloat16)

    def contract(x, c, held, part):
        more = lax.dot_general(
            held[...],
            flat_ref[:, c * width + x : c * width + x + WIDE],
            (((1,), (1,)), ((), ())),
            preferred_element_type=jnp.float32,
        )
        return more if part is None else part + more

    def finish(group, part):
        for kk in range(GROUP):
            k = group * GROUP + kk
            rows_ref[pl.ds(k, total, stride=count), :] = part[kk * total : (kk + 1) * total].T

    helds = (held_a, held_b)
    work = [(g, x, c) for g in range(count // GROUP) for x in range(0, width, WIDE) for c in range(comps)]
    each = len(work) // (count // GROUP)
    build(*work[0], helds[0])
    part = None
    for n, (g, x, c) in enumerate(work):
        if n + 1 < len(work):
            build(*work[n + 1], helds[(n + 1) % 2])
        part = contract(x, c, helds[n % 2], part)
        if n % each == each - 1:
            finish(g, part)
            part = None
    size = out_ref.shape[1]
    each = out_ref.shape[0] // blocks
    for r in range(blocks):
        rows = rows_ref[r * each * size : (r + 1) * each * size, :].astype(jnp.bfloat16)
        out_ref[pl.ds(absolute(r) * each, each)] = rows.reshape(each, size, total)


def local_tensor(grads, own, other, early, shards, absolute):
    chips, comps, count, width = own.shape
    total = 2 * chips * count
    return pl.pallas_call(
        lambda *refs: tensor_kernel(absolute, *refs),
        out_shape=jax.ShapeDtypeStruct((shards, total * count // shards, total), jnp.bfloat16),
        in_specs=[pl.BlockSpec(memory_space=pltpu.VMEM)] * (3 + EARLY),
        out_specs=pl.BlockSpec(memory_space=pltpu.VMEM),
        scratch_shapes=[
            pltpu.VMEM((comps, total, width), jnp.float32),
            pltpu.VMEM((total, comps * width), jnp.bfloat16),
            pltpu.VMEM((GROUP * total, WIDE), jnp.bfloat16),
            pltpu.VMEM((GROUP * total, WIDE), jnp.bfloat16),
            pltpu.VMEM((count * total, total), jnp.float32),
        ],
        compiler_params=pltpu.CompilerParams(vmem_limit_bytes=16 << 20),
        cost_estimate=pl.CostEstimate(flops=1_700_000_000, bytes_accessed=2_000_000, transcendentals=0),
        name="tensor",
    )(grads, own, other, *early)


def placed_kernel(relative, tiles_ref, out_ref):
    total = tiles_ref[0].astype(jnp.float32)
    for i in range(1, tiles_ref.shape[0]):
        total = total + tiles_ref[i].astype(jnp.float32)
    count, pairs, modes = out_ref.shape
    place = lax.broadcasted_iota(jnp.int32, (8, modes), 1)
    lane = relative(place >> 4) * 16 + (place & 15)
    for i in range(pairs):
        for r in range(0, count, 8):
            out_ref[r : r + 8, i, :] = picked(total[i * count + r : i * count + r + 8], lane)


def placed(tiles, count, relative):
    rows, total = tiles.shape[1:]
    return pl.pallas_call(
        lambda *refs: placed_kernel(relative, *refs),
        out_shape=jax.ShapeDtypeStruct((count, rows // count, total), jnp.float32),
        in_specs=[pl.BlockSpec(memory_space=pltpu.VMEM)],
        out_specs=pl.BlockSpec(memory_space=pltpu.VMEM),
        compiler_params=pltpu.CompilerParams(vmem_limit_bytes=4 << 20),
        name="placed",
    )(tiles)


def local(modes, stencil_coef, volumes, neighbours):
    _, count, width = modes.shape
    cells = width * lax.axis_size(SPACE)
    low = modes.astype(jnp.bfloat16)
    chips = lax.axis_size("yhi")
    copies = jnp.broadcast_to(low, (chips, *low.shape))
    own = lax.all_to_all(copies, "yhi", 0, 0, tiled=True)
    shards = lax.axis_size(SPACE)
    head, tail = modes[:, :, :LANES], modes[:, :, width - LANES :]
    odd = lax.axis_index("x") % 2 == 1
    evens = [(i, i + 1) for i in range(0, shards, 2)]
    odds = [(i, i + 1) for i in range(1, shards - 1, 2)]
    left = lax.ppermute(jnp.where(odd, head, tail), SPACE, evens + [(b, a) for a, b in evens])
    right = lax.ppermute(jnp.where(odd, tail, head), SPACE, odds + [(b, a) for a, b in odds])
    grads = weighted_grads(modes, left, right, stencil_coef, volumes, neighbours, 1.0 / math.sqrt(cells))
    own, grads = lax.optimization_barrier((own, grads))
    early = early_part(grads, own)
    other = lax.ppermute(own, "core", [(0, 1), (1, 0)])

    def swapped(block):
        return block ^ lax.axis_index("core")

    absolute, relative = swapped, swapped
    share = local_tensor(grads, own, other, early, lax.axis_size(SPACE), absolute)
    tiles = lax.all_to_all(share, SPACE, 0, 0, tiled=True)
    return placed(tiles, count, relative)


def solution(mesh):
    sizes = (8, 2, 4, 4, 2)
    fine = Mesh(mesh.devices.reshape(sizes), SPACE + MODE)
    in_specs = (P(None, MODE, SPACE), P(None, None, SPACE), P(SPACE), P(None, SPACE))
    out_specs = P(MODE, SPACE, None)
    return jax.shard_map(local, mesh=fine, in_specs=in_specs, out_specs=out_specs, check_vma=False)
```
